32 devices in a mesh: groups: 2 (over y), seq: 8 (over z, x), vocab: 1, batch: 2 (over core).
Axes of the slice: x: 2, y: 2, z: 4, core: 2. Of those that a mesh axis runs over, the one named last changes fastest.
Arguments:
- queries: bfloat16 [4, 1536, 3584], P(('groups', 'vocab', 'batch'), 'seq'), parts along dimension 0, may hold values from -300 to 300
- keys: bfloat16 [4, 1536, 512], P(('groups', 'vocab', 'batch'), 'seq'), parts along dimension 0, may hold values from -10 to 10
- values: bfloat16 [4, 1536, 512], P(('groups', 'vocab', 'batch'), 'seq'), parts along dimension 0, may hold values from -24 to 24
- residual: bfloat16 [4, 1536, 3584], P(('groups', 'vocab', 'batch'), 'seq'), parts along dimension 0, may hold values from -2048 to 2048
- norm_gain: float32 [3584], replicated, may hold values from 0.5 to 1.5
Outputs:
- normed: bfloat16 [4, 1536, 3584], P(('groups', 'vocab', 'batch'), 'seq'), parts along dimension 0
The draws below stay inside these ranges and needn't reach their ends.
There are 2 independent parts, one for each index of `groups`. The reference program is written for one: setup_inputs(seed, part) draws one part's arguments, and reference() takes and returns one part's arrays. A program takes and returns all parts, laid end to end along the dimension named above; an argument that names none is the same for every part. Nothing has to cross between parts.
All inputs are finite; a program needn't handle non-finite values.
Results may differ from the reference program's by a relative error of at most 0.0049.
Values may be sent and summed in bfloat16 or wider, within the bound.
A program may use at most 128 MiB of HBM per device.

```python
import math
import jax
import jax.numpy as jnp
from jax import lax

D = 3584
QUERY_HEADS = 28
KEY_VALUE_HEADS = 4
HEAD_WIDTH = 128
RESPONSE_LENGTH = 1536
RESPONSE_COUNT = 2


def query_keys(key):
    key_start, key_query = jax.random.split(jax.random.fold_in(key, 11), 2)
    unscaled_keys = 1.5 * jax.random.truncated_normal(key_start, -6.0, 6.0, (RESPONSE_COUNT, RESPONSE_LENGTH, KEY_VALUE_HEADS, HEAD_WIDTH), jnp.float32)
    unscaled_query = 1.5 * jax.random.truncated_normal(key_query, -6.0, 6.0, (RESPONSE_COUNT, RESPONSE_LENGTH, QUERY_HEADS, HEAD_WIDTH), jnp.float32)
    return (unscaled_query.reshape(RESPONSE_COUNT, RESPONSE_LENGTH, QUERY_HEADS * HEAD_WIDTH), unscaled_keys.reshape(RESPONSE_COUNT, RESPONSE_LENGTH, KEY_VALUE_HEADS * HEAD_WIDTH))


def draw_queries(key, part):
    return query_keys(key)[0].astype(jnp.bfloat16)


def draw_keys(key, part):
    return query_keys(key)[1].astype(jnp.bfloat16)


def draw_residual(key, part):
    key_rows, key_columns, key_start = jax.random.split(jax.random.fold_in(key, 23), 3)
    row_scale = jnp.exp(jax.random.uniform(key_rows, (RESPONSE_COUNT, RESPONSE_LENGTH, 1), jnp.float32, math.log(0.3), math.log(3.0)))
    column_scale = jnp.exp(jax.random.uniform(key_columns, (1, 1, D), jnp.float32, math.log(0.3), math.log(3.0)))
    drawn = jax.random.truncated_normal(key_start, -6.0, 6.0, (RESPONSE_COUNT, RESPONSE_LENGTH, D), jnp.float32) * row_scale * column_scale
    return drawn.astype(jnp.bfloat16)


def block_levels(stream_key, dims, pieces, low, high):
    factor_of = 1.0
    for axis_at, parts in pieces:
        heights = jax.random.uniform(jax.random.fold_in(jax.random.fold_in(stream_key, 6), axis_at), (parts,), jnp.float32, low / len(pieces), high / len(pieces))
        factor_of = factor_of * jnp.repeat(jnp.exp(heights), dims[axis_at] // parts).reshape((-1,) + (1,) * (len(dims) - 1 - axis_at))
    return factor_of


def scatter_about(rng, shape, spread, bound, shards=(), held_as=jnp.bfloat16):
    gain = block_levels(rng, shape, shards, -0.22, 0.18) if shards else 1.0
    values = jax.random.normal(rng, shape, jnp.float32) * spread * gain
    return jnp.minimum(jnp.maximum(values, -bound), bound).astype(held_as)


def setup_inputs(seed: int = 0, part: int = 0) -> dict:
    splits = jax.random.split(jax.random.key(seed), 6)
    part_splits = jax.random.split(jax.random.fold_in(splits[5], part), 6)
    queries = draw_queries(jax.random.fold_in(jax.random.fold_in(splits[5], part), 71), part)
    keys = draw_keys(jax.random.fold_in(jax.random.fold_in(splits[5], part), 71), part)
    values = scatter_about(part_splits[2], (RESPONSE_COUNT, RESPONSE_LENGTH, KEY_VALUE_HEADS * HEAD_WIDTH), 4.0, 24.0, ((0, 2), (1, 8)))
    residual = draw_residual(jax.random.fold_in(jax.random.fold_in(splits[5], part), 71), part)
    norm_gain = jnp.clip(1.0 + 0.1 * jax.random.normal(splits[4], (D,), jnp.float32), 0.5, 1.5)
    return dict(queries=queries, keys=keys, values=values, residual=residual, norm_gain=norm_gain)


norm_eps = 1e-06

def reference(queries, keys, values, residual, norm_gain):
    queries_per_group = QUERY_HEADS // KEY_VALUE_HEADS
    position = jnp.arange(RESPONSE_LENGTH, dtype=jnp.int32)
    causal = position[None, :] <= position[:, None]

    def one_response(inputs):
        query_all, key_all, value_all = inputs

        def one_head(head_index):
            group_index = head_index // queries_per_group
            query_head = lax.dynamic_slice_in_dim(query_all, (head_index * HEAD_WIDTH).astype(jnp.int32), HEAD_WIDTH, 1)
            key_head = lax.dynamic_slice_in_dim(key_all, (group_index * HEAD_WIDTH).astype(jnp.int32), HEAD_WIDTH, 1)
            value_head = lax.dynamic_slice_in_dim(value_all, (group_index * HEAD_WIDTH).astype(jnp.int32), HEAD_WIDTH, 1)
            scores = jnp.dot(query_head, key_head.T, preferred_element_type=jnp.float32) * (1.0 / math.sqrt(HEAD_WIDTH))
            scores = jnp.where(causal, scores, -jnp.inf)
            row_max = lax.optimization_barrier(jnp.max(scores, axis=1, keepdims=True))
            weights = jnp.exp(scores - row_max)
            soft_probs = (weights / lax.optimization_barrier(jnp.sum(weights, axis=1, keepdims=True))).astype(jnp.bfloat16)
            return jnp.dot(soft_probs, value_head, preferred_element_type=jnp.float32).astype(jnp.bfloat16)
        heads_out = lax.map(one_head, jnp.arange(QUERY_HEADS, dtype=jnp.int32))
        return jnp.transpose(heads_out, (1, 0, 2)).reshape(RESPONSE_LENGTH, QUERY_HEADS * HEAD_WIDTH)
    attended = lax.map(one_response, (queries, keys, values))

    def one_norm(inputs):
        attended_rows, residual_rows = inputs
        hidden = residual_rows.astype(jnp.float32) + attended_rows.astype(jnp.float32)
        inv_rms = lax.rsqrt(lax.optimization_barrier(jnp.mean(hidden * hidden, axis=1, keepdims=True)) + norm_eps)
        return (hidden * inv_rms * norm_gain).astype(jnp.bfloat16)
    return lax.map(one_norm, (attended, residual))
```

```python
import functools
import math

import jax
import jax.numpy as jnp
from jax import lax
from jax.experimental import pallas as pl
from jax.experimental.pallas import tpu as pltpu
from jax.sharding import PartitionSpec as P

HEAD_WIDTH = 128
norm_eps = 1e-06
MESH = pl.DeviceIdType.MESH


def kernel(
    planes,
    rows,
    kv_heads,
    per_group,
    q_hbm,
    k_hbm,
    v_hbm,
    r_hbm,
    gain_ref,
    out_ref,
    qbuf,
    rbuf,
    kvbuf,
    top,
    acc,
    local_sem,
    up_send,
    up_recv,
    side_send,
    side_recv,
):
    W = HEAD_WIDTH
    width = kv_heads * per_group * W
    me = lax.axis_index("seq")
    plane = me // 2
    col = lax.rem(me, 2)
    above = me + 2
    below = me - 2
    side = me + 1 - 2 * col
    has_up = plane + 1 < planes
    has_down = plane > 0
    factor = math.log2(math.e) / math.sqrt(W)

    def own_copy(kind, src):
        return pltpu.make_async_copy(src.at[0], kvbuf.at[kind, me], local_sem.at[kind])

    own_k = own_copy(0, k_hbm)
    own_v = own_copy(1, v_hbm)
    q_in = pltpu.make_async_copy(q_hbm.at[0], qbuf, local_sem.at[2])
    r_in = pltpu.make_async_copy(r_hbm.at[0], rbuf, local_sem.at[3])
    own_k.start()
    own_v.start()
    q_in.start()
    r_in.start()

    barrier = pltpu.get_barrier_semaphore()
    pl.semaphore_signal(barrier, inc=1, device_id={"seq": side}, device_id_type=MESH)

    @pl.when(has_up)
    def _():
        pl.semaphore_signal(barrier, inc=1, device_id={"seq": above}, device_id_type=MESH)

    @pl.when(has_down)
    def _():
        pl.semaphore_signal(barrier, inc=1, device_id={"seq": below}, device_id_type=MESH)

    pl.semaphore_wait(barrier, 1 + has_up.astype(jnp.int32) + has_down.astype(jnp.int32))

    def up_copy(kind, q, column):
        slot = kvbuf.at[kind, 2 * q + column]
        return pltpu.make_async_remote_copy(
            src_ref=slot,
            dst_ref=slot,
            send_sem=up_send.at[kind, q],
            recv_sem=up_recv.at[kind, q],
            device_id={"seq": above},
            device_id_type=MESH,
        )

    def side_copy(kind, q, column):
        slot = kvbuf.at[kind, 2 * q + column]
        return pltpu.make_async_remote_copy(
            src_ref=slot,
            dst_ref=slot,
            send_sem=side_send.at[kind, q],
            recv_sem=side_recv.at[kind, q],
            device_id={"seq": side},
            device_id_type=MESH,
        )

    for kind, own in ((0, own_k), (1, own_v)):
        own.wait()

        @pl.when(has_up)
        def _(kind=kind):
            up_copy(kind, plane, col).start()

        @pl.when(col == 0)
        def _(kind=kind):
            side_copy(kind, plane, col).start()

    @pl.when(col == 0)
    def _():
        kvbuf[0, me + 1] = jnp.zeros((rows, kv_heads * W), jnp.bfloat16)
        kvbuf[1, me + 1] = jnp.zeros((rows, kv_heads * W), jnp.bfloat16)

    q_in.wait()

    def relay(q):
        for kind in (0, 1):
            up_copy(kind, q, col).wait_recv()

            @pl.when(has_up)
            def _(kind=kind):
                up_copy(kind, q, col).start()

            side_copy(kind, q, col).start()

    def attend(q, first):
        def one_group(g, carry):
            lanes = pl.ds(pl.multiple_of(g * W, W), W)
            keys = kvbuf[0, pl.ds(2 * q, 2), :, lanes].reshape(2 * rows, W)
            vals = kvbuf[1, pl.ds(2 * q, 2), :, lanes].reshape(2 * rows, W)
            vals = jnp.concatenate([vals, jnp.ones_like(vals)], axis=1)
            for j in range(per_group):
                head = g * per_group + j
                query = qbuf[:, pl.ds(pl.multiple_of(head * W, W), W)]
                s = lax.dot_general(
                    query, keys, (((1,), (1,)), ((), ())), preferred_element_type=jnp.float32
                )
                if first:
                    at_row = lax.broadcasted_iota(jnp.int32, s.shape, 0) + col * rows
                    at_key = lax.broadcasted_iota(jnp.int32, s.shape, 1)
                    s = jnp.where(at_key <= at_row, s, -jnp.inf)
                high = jnp.max(s, axis=1, keepdims=True)
                if not first:
                    old = top[head]
                    high = jnp.maximum(old[:, :1], high)
                w = jnp.exp2((s - high) * factor).astype(jnp.bfloat16)
                o = jnp.dot(w, vals, preferred_element_type=jnp.float32)
                wide = jnp.broadcast_to(high, (rows, W))
                if not first:
                    fade = jnp.exp2((old - wide) * factor)
                    o = o + acc[head] * jnp.concatenate([fade, fade], axis=1)
                top[head] = wide
                acc[head] = o
            return carry

        lax.fori_loop(0, kv_heads, one_group, 0)

    @pl.when(has_down)
    def _():
        relay(plane - 1)

    @pl.when(col == 1)
    def _():
        side_copy(0, plane, 1 - col).wait_recv()
        side_copy(1, plane, 1 - col).wait_recv()

    attend(plane, True)

    def step(t, carry):
        @pl.when(t <= plane)
        def _():
            relay(plane - t)

        q = plane - t + 1
        side_copy(0, q, 1 - col).wait_recv()
        side_copy(1, q, 1 - col).wait_recv()
        attend(q, False)
        return carry

    lax.fori_loop(2, plane + 2, step, 0)

    r_in.wait()
    total = jnp.zeros((rows, W), jnp.float32)
    for head in range(kv_heads * per_group):
        lanes = slice(head * W, (head + 1) * W)
        both = acc[head]
        attended = (both[:, :W] / both[:, W:]).astype(jnp.bfloat16).astype(jnp.float32)
        hidden = rbuf[:, lanes].astype(jnp.float32) + attended
        total = total + hidden * hidden
        top[head] = hidden
    mean = jnp.sum(total, axis=1, keepdims=True) / width
    scale = jnp.broadcast_to(lax.rsqrt(mean + norm_eps), (rows, W))
    for head in range(kv_heads * per_group):
        lanes = slice(head * W, (head + 1) * W)
        out_ref[0, :, lanes] = (top[head] * scale * gain_ref[:, lanes]).astype(jnp.bfloat16)

    for kind in (0, 1):

        @pl.when(has_up)
        def _(kind=kind):
            up_copy(kind, plane, col).wait_send()

        @pl.when(col == 0)
        def _(kind=kind):
            side_copy(kind, plane, col).wait_send()

    def drain(q, carry):
        for kind in (0, 1):

            @pl.when(has_up)
            def _(kind=kind):
                up_copy(kind, q, col).wait_send()

            side_copy(kind, q, col).wait_send()
        return carry

    lax.fori_loop(0, plane, drain, 0)


def body(queries, keys, values, residual, norm_gain):
    count = lax.axis_size("seq")
    rows = queries.shape[1]
    width = queries.shape[2]
    kv_heads = keys.shape[2] // HEAD_WIDTH
    heads = width // HEAD_WIDTH
    planes = count // 2
    hbm = pl.BlockSpec(memory_space=pl.ANY)
    vmem = pl.BlockSpec(memory_space=pltpu.VMEM)
    return pl.pallas_call(
        functools.partial(kernel, planes, rows, kv_heads, heads // kv_heads),
        out_shape=jax.ShapeDtypeStruct(queries.shape, jnp.bfloat16),
        in_specs=[hbm, hbm, hbm, hbm, vmem],
        out_specs=vmem,
        scratch_shapes=[
            pltpu.VMEM((rows, width), jnp.bfloat16),
            pltpu.VMEM((rows, width), jnp.bfloat16),
            pltpu.VMEM((2, count, rows, keys.shape[2]), jnp.bfloat16),
            pltpu.VMEM((heads, rows, HEAD_WIDTH), jnp.float32),
            pltpu.VMEM((heads, rows, 2 * HEAD_WIDTH), jnp.float32),
            pltpu.SemaphoreType.DMA((4,)),
            pltpu.SemaphoreType.DMA((2, planes)),
            pltpu.SemaphoreType.DMA((2, planes)),
            pltpu.SemaphoreType.DMA((2, planes)),
            pltpu.SemaphoreType.DMA((2, planes)),
        ],
        compiler_params=pltpu.CompilerParams(
            collective_id=0, has_side_effects=True, vmem_limit_bytes=48 * 1024 * 1024
        ),
    )(queries, keys, values, residual, norm_gain.reshape(1, width))


def solution(mesh):
    rows = P(("groups", "vocab", "batch"), "seq", None)
    return jax.shard_map(
        body,
        mesh=mesh,
        in_specs=(rows, rows, rows, rows, P()),
        out_specs=rows,
        check_vma=False,
    )
```

```python
import functools
import math

import jax
import jax.numpy as jnp
from jax import lax
from jax.experimental import pallas as pl
from jax.experimental.pallas import tpu as pltpu
from jax.sharding import PartitionSpec as P

HEAD_WIDTH = 128
norm_eps = 1e-06
MESH = pl.DeviceIdType.MESH


def kernel(
    planes,
    rows,
    kv_heads,
    per_group,
    q_hbm,
    k_hbm,
    v_hbm,
    r_hbm,
    gain_ref,
    out_ref,
    qbuf,
    rbuf,
    kvbuf,
    top,
    acc,
    squares,
    local_sem,
    own_sem,
    up_send,
    up_recv,
    side_send,
    side_recv,
    extra_send,
    extra_recv,
):
    W = HEAD_WIDTH
    width = kv_heads * per_group * W
    half = kv_heads // 2
    me = lax.axis_index("seq")
    plane = me // 2
    col = lax.rem(me, 2)
    above = me + 2
    below = me - 2
    side = me + 1 - 2 * col
    has_up = plane + 1 < planes
    has_down = plane > 0
    factor = math.log2(math.e) / math.sqrt(W)

    own = []
    for g in range(kv_heads):
        for kind, src in ((0, k_hbm), (1, v_hbm)):
            copy = pltpu.make_async_copy(
                src.at[0, :, pl.ds(g * W, W)],
                kvbuf.at[g, me, :, pl.ds(kind * W, W)],
                own_sem.at[g, kind],
            )
            copy.start()
            own.append(copy)
    q_in = pltpu.make_async_copy(q_hbm.at[0], qbuf, local_sem.at[0])
    r_in = pltpu.make_async_copy(r_hbm.at[0], rbuf, local_sem.at[1])
    q_in.start()
    r_in.start()

    barrier = pltpu.get_barrier_semaphore()
    pl.semaphore_signal(barrier, inc=1, device_id={"seq": side}, device_id_type=MESH)

    @pl.when(has_up)
    def _():
        pl.semaphore_signal(barrier, inc=1, device_id={"seq": above}, device_id_type=MESH)

    @pl.when(has_down)
    def _():
        pl.semaphore_signal(barrier, inc=1, device_id={"seq": below}, device_id_type=MESH)

    pl.semaphore_wait(barrier, 1 + has_up.astype(jnp.int32) + has_down.astype(jnp.int32))

    def remote(slot, send_sem, recv_sem, target):
        return pltpu.make_async_remote_copy(
            src_ref=slot,
            dst_ref=slot,
            send_sem=send_sem,
            recv_sem=recv_sem,
            device_id={"seq": target},
            device_id_type=MESH,
        )

    def up_copy(g, q):
        return remote(kvbuf.at[g, 2 * q + col], up_send.at[g, q], up_recv.at[g, q], above)

    def side_copy(g, q, column):
        return remote(kvbuf.at[g, 2 * q + column], side_send.at[g, q], side_recv.at[g, q], side)

    def extra_copy(g, q):
        return remote(kvbuf.at[g, 2 * q], extra_send.at[g], extra_recv.at[g], above)

    def by_extra(g, q, column):
        return (column == 1) & (q == plane - 1) & (g >= half)

    for g in range(kv_heads):
        own[2 * g].wait()
        own[2 * g + 1].wait()

        @pl.when(has_up)
        def _(g=g):
            up_copy(g, plane).start()

        @pl.when(col == 0)
        def _(g=g):
            side_copy(g, plane, col).start()

    @pl.when(col == 0)
    def _():
        for g in range(kv_heads):
            kvbuf[g, me + 1] = jnp.zeros((rows, 2 * W), jnp.bfloat16)

    squares[...] = jnp.zeros_like(squares)
    q_in.wait()
    r_in.wait()

    def relay(g, q):
        up_copy(g, q).wait_recv()

        @pl.when(has_up)
        def _():
            up_copy(g, q).start()

        @pl.when(jnp.logical_not(by_extra(g, q, 1 - col)))
        def _():
            side_copy(g, q, col).start()

    def attend(g, q, first):
        keys = kvbuf[g, pl.ds(2 * q, 2), :, :W].reshape(2 * rows, W)
        vals = kvbuf[g, pl.ds(2 * q, 2), :, W:].reshape(2 * rows, W)
        vals = jnp.concatenate([vals, jnp.ones_like(vals)], axis=1)
        for j in range(per_group):
            head = g * per_group + j
            query = qbuf[:, pl.ds(pl.multiple_of(head * W, W), W)]
            s = lax.dot_general(
                query, keys, (((1,), (1,)), ((), ())), preferred_element_type=jnp.float32
            )
            if first:
                at_row = lax.broadcasted_iota(jnp.int32, s.shape, 0) + col * rows
                at_key = lax.broadcasted_iota(jnp.int32, s.shape, 1)
                s = jnp.where(at_key <= at_row, s, -jnp.inf)
            high = jnp.max(s, axis=1, keepdims=True)
            if not first:
                old = top[head]
                high = jnp.maximum(old[:, :1], high)
            w = jnp.exp2((s - high) * factor).astype(jnp.bfloat16)
            o = jnp.dot(w, vals, preferred_element_type=jnp.float32)
            wide = jnp.broadcast_to(high, (rows, W))
            if not first:
                fade = jnp.exp2((old - wide) * factor)
                o = o + acc[head] * jnp.concatenate([fade, fade], axis=1)
            top[head] = wide
            acc[head] = o

    def finish(g):
        total = squares[...]
        for j in range(per_group):
            head = g * per_group + j
            lanes = pl.ds(pl.multiple_of(head * W, W), W)
            both = acc[head]
            attended = (both[:, :W] / both[:, W:]).astype(jnp.bfloat16).astype(jnp.float32)
            hidden = rbuf[:, lanes].astype(jnp.float32) + attended
            total = total + hidden * hidden
            top[head] = hidden
        squares[...] = total

    def diagonal(g, carry):
        @pl.when(has_down)
        def _():
            relay(g, plane - 1)

        @pl.when(col == 1)
        def _():
            side_copy(g, plane, 1 - col).wait_recv()

        @pl.when((col == 1) & has_up & (g >= half))
        def _():
            extra_copy(g, plane).start()

        attend(g, plane, True)

        @pl.when(plane == 0)
        def _():
            finish(g)

        return carry

    lax.fori_loop(0, kv_heads, diagonal, 0)

    def step(t, carry):
        q = plane - t + 1

        def one(g, inner):
            @pl.when(t <= plane)
            def _():
                relay(g, q - 1)

            @pl.when(by_extra(g, q, col))
            def _():
                extra_copy(g, q).wait_recv()

            @pl.when(jnp.logical_not(by_extra(g, q, col)))
            def _():
                side_copy(g, q, 1 - col).wait_recv()

            attend(g, q, False)

            @pl.when(q == 0)
            def _():
                finish(g)

            return inner

        return lax.fori_loop(0, kv_heads, one, carry)

    lax.fori_loop(2, plane + 2, step, 0)

    mean = jnp.sum(squares[...], axis=1, keepdims=True) / width
    scale = jnp.broadcast_to(lax.rsqrt(mean + norm_eps), (rows, W))
    for head in range(kv_heads * per_group):
        lanes = slice(head * W, (head + 1) * W)
        gain = gain_ref[lanes].reshape(1, W)
        out_ref[0, :, lanes] = (top[head] * scale * gain).astype(jnp.bfloat16)

    def drain_own(g, carry):
        @pl.when(has_up)
        def _():
            up_copy(g, plane).wait_send()

        @pl.when(col == 0)
        def _():
            side_copy(g, plane, col).wait_send()

        @pl.when((col == 1) & has_up & (g >= half))
        def _():
            extra_copy(g, plane).wait_send()

        return carry

    lax.fori_loop(0, kv_heads, drain_own, 0)

    def drain(q, carry):
        def one(g, inner):
            @pl.when(has_up)
            def _():
                up_copy(g, q).wait_send()

            @pl.when(jnp.logical_not(by_extra(g, q, 1 - col)))
            def _():
                side_copy(g, q, col).wait_send()

            return inner

        return lax.fori_loop(0, kv_heads, one, carry)

    lax.fori_loop(0, plane, drain, 0)


def body(queries, keys, values, residual, norm_gain):
    count = lax.axis_size("seq")
    rows = queries.shape[1]
    width = queries.shape[2]
    kv_heads = keys.shape[2] // HEAD_WIDTH
    heads = width // HEAD_WIDTH
    planes = count // 2
    hbm = pl.BlockSpec(memory_space=pltpu.HBM)
    vmem = pl.BlockSpec(memory_space=pltpu.VMEM)
    return pl.pallas_call(
        functools.partial(kernel, planes, rows, kv_heads, heads // kv_heads),
        out_shape=jax.ShapeDtypeStruct(queries.shape, jnp.bfloat16),
        in_specs=[hbm, hbm, hbm, hbm, vmem],
        out_specs=vmem,
        scratch_shapes=[
            pltpu.VMEM((rows, width), jnp.bfloat16),
            pltpu.VMEM((rows, width), jnp.bfloat16),
            pltpu.VMEM((kv_heads, count, rows, 2 * HEAD_WIDTH), jnp.bfloat16),
            pltpu.VMEM((heads, rows, HEAD_WIDTH), jnp.float32),
            pltpu.VMEM((heads, rows, 2 * HEAD_WIDTH), jnp.float32),
            pltpu.VMEM((rows, HEAD_WIDTH), jnp.float32),
            pltpu.SemaphoreType.DMA((2,)),
            pltpu.SemaphoreType.DMA((kv_heads, 2)),
            pltpu.SemaphoreType.DMA((kv_heads, planes)),
            pltpu.SemaphoreType.DMA((kv_heads, planes)),
            pltpu.SemaphoreType.DMA((kv_heads, planes)),
            pltpu.SemaphoreType.DMA((kv_heads, planes)),
            pltpu.SemaphoreType.DMA((kv_heads,)),
            pltpu.SemaphoreType.DMA((kv_heads,)),
        ],
        compiler_params=pltpu.CompilerParams(
            collective_id=0, has_side_effects=True, vmem_limit_bytes=48 * 1024 * 1024
        ),
    )(queries, keys, values, residual, norm_gain)


def solution(mesh):
    rows = P(("groups", "vocab", "batch"), "seq", None)
    return jax.shard_map(
        body,
        mesh=mesh,
        in_specs=(rows, rows, rows, rows, P()),
        out_specs=rows,
        check_vma=False,
    )
```

```python
import functools
import math

import jax
import jax.numpy as jnp
from jax import lax
from jax.experimental import pallas as pl
from jax.experimental.pallas import tpu as pltpu
from jax.sharding import PartitionSpec as P

HEAD_WIDTH = 128
norm_eps = 1e-06
MESH = pl.DeviceIdType.MESH


def kernel(
    planes,
    rows,
    kv_heads,
    per_group,
    q_hbm,
    k_hbm,
    v_hbm,
    r_hbm,
    gain_ref,
    out_ref,
    qbuf,
    rbuf,
    kvbuf,
    top,
    acc,
    squares,
    local_sem,
    own_sem,
    up_send,
    up_recv,
    side_send,
    side_recv,
    extra_send,
    extra_recv,
):
    W = HEAD_WIDTH
    width = kv_heads * per_group * W
    me = lax.axis_index("seq")
    plane = me // 2
    col = lax.rem(me, 2)
    above = me + 2
    below = me - 2
    side = me + 1 - 2 * col
    has_up = plane + 1 < planes
    has_down = plane > 0
    factor = math.log2(math.e) / math.sqrt(W)

    own = []
    for g in range(kv_heads):
        for kind, src in ((0, k_hbm), (1, v_hbm)):
            copy = pltpu.make_async_copy(
                src.at[0, :, pl.ds(g * W, W)],
                kvbuf.at[g, me, :, pl.ds(kind * W, W)],
                own_sem.at[g, kind],
            )
            copy.start()
            own.append(copy)
    heads = kv_heads * per_group

    def query_copy(head):
        lanes = pl.ds(pl.multiple_of(head * W, W), W)
        return pltpu.make_async_copy(
            q_hbm.at[0, :, lanes], qbuf.at[head], local_sem.at[head]
        )

    lax.fori_loop(0, heads, lambda head, carry: query_copy(head).start(), None)
    r_in = pltpu.make_async_copy(r_hbm.at[0], rbuf, local_sem.at[heads])
    r_in.start()

    barrier = pltpu.get_barrier_semaphore()
    pl.semaphore_signal(barrier, inc=1, device_id={"seq": side}, device_id_type=MESH)

    @pl.when(has_up)
    def _():
        pl.semaphore_signal(barrier, inc=1, device_id={"seq": above}, device_id_type=MESH)

    @pl.when(has_down)
    def _():
        pl.semaphore_signal(barrier, inc=1, device_id={"seq": below}, device_id_type=MESH)

    pl.semaphore_wait(barrier, 1 + has_up.astype(jnp.int32) + has_down.astype(jnp.int32))

    def remote(slot, send_sem, recv_sem, target):
        return pltpu.make_async_remote_copy(
            src_ref=slot,
            dst_ref=slot,
            send_sem=send_sem,
            recv_sem=recv_sem,
            device_id={"seq": target},
            device_id_type=MESH,
        )

    def up_copy(g, q):
        return remote(kvbuf.at[g, 2 * q + col], up_send.at[g, q], up_recv.at[g, q], above)

    def side_copy(g, q, column):
        return remote(kvbuf.at[g, 2 * q + column], side_send.at[g, q], side_recv.at[g, q], side)

    def extra_copy(g):
        return remote(kvbuf.at[g, 0], extra_send.at[g], extra_recv.at[g], above)

    def by_extra(g, q, column):
        return (column == 1) & (q == 0) & has_down & (lax.rem(g, 2) == 1)

    for g in range(kv_heads):
        own[2 * g].wait()
        own[2 * g + 1].wait()

        @pl.when(has_up)
        def _(g=g):
            up_copy(g, plane).start()

        @pl.when(col == 0)
        def _(g=g):
            side_copy(g, plane, col).start()

    @pl.when(col == 0)
    def _():
        for g in range(kv_heads):
            kvbuf[g, me + 1] = jnp.zeros((rows, 2 * W), jnp.bfloat16)

    squares[...] = jnp.zeros_like(squares)
    lax.fori_loop(0, heads, lambda head, carry: query_copy(head).wait(), None)
    r_in.wait()

    def relay(g, q):
        up_copy(g, q).wait_recv()

        @pl.when(has_up)
        def _():
            up_copy(g, q).start()

        @pl.when(jnp.logical_not(by_extra(g, q, 1 - col)))
        def _():
            side_copy(g, q, col).start()

    def attend(g, q, first):
        keys = kvbuf[g, pl.ds(2 * q, 2), :, :W].reshape(2 * rows, W)
        vals = kvbuf[g, pl.ds(2 * q, 2), :, W:].reshape(2 * rows, W)
        vals = jnp.concatenate([vals, jnp.ones_like(vals)], axis=1)

        def scores(j):
            return lax.dot_general(
                qbuf[g * per_group + j],
                keys,
                (((1,), (1,)), ((), ())),
                preferred_element_type=jnp.float32,
            )

        s_next = scores(0)
        for j in range(per_group):
            head = g * per_group + j
            s = s_next
            if j + 1 < per_group:
                s_next = scores(j + 1)
            if first:
                at_row = lax.broadcasted_iota(jnp.int32, s.shape, 0) + col * rows
                at_key = lax.broadcasted_iota(jnp.int32, s.shape, 1)
                s = jnp.where(at_key <= at_row, s, -jnp.inf)
            wide = jnp.broadcast_to(jnp.max(s, axis=1, keepdims=True), (rows, W))
            if not first:
                old = top[head]
                wide = jnp.maximum(old, wide)
            s = (s - jnp.concatenate([wide] * (2 * rows // W), axis=1)) * factor
            w = jnp.exp2(s).astype(jnp.bfloat16)
            o = jnp.dot(w, vals, preferred_element_type=jnp.float32)
            if not first:
                fade = jnp.exp2((old - wide) * factor)
                o = o + acc[head] * jnp.concatenate([fade, fade], axis=1)
            top[head] = wide
            acc[head] = o

    def finish(g):
        total = squares[...]
        for j in range(per_group):
            head = g * per_group + j
            lanes = pl.ds(pl.multiple_of(head * W, W), W)
            both = acc[head]
            attended = (both[:, :W] / both[:, W:]).astype(jnp.bfloat16).astype(jnp.float32)
            hidden = rbuf[:, lanes].astype(jnp.float32) + attended
            total = total + hidden * hidden
            top[head] = hidden
        squares[...] = total

    def diagonal(g, carry):
        @pl.when(has_down)
        def _():
            relay(g, plane - 1)

        @pl.when(col == 1)
        def _():
            side_copy(g, plane, 1 - col).wait_recv()

        @pl.when((col == 1) & (plane == 0) & has_up & (lax.rem(g, 2) == 1))
        def _():
            extra_copy(g).start()

        attend(g, plane, True)

        @pl.when(plane == 0)
        def _():
            finish(g)

        return carry

    lax.fori_loop(0, kv_heads, diagonal, 0)

    def step(t, carry):
        q = plane - t + 1

        def one(g, inner):
            @pl.when(t <= plane)
            def _():
                relay(g, q - 1)

            @pl.when(by_extra(g, q, col))
            def _():
                extra_copy(g).wait_recv()

            @pl.when(by_extra(g, q, col) & has_up)
            def _():
                extra_copy(g).start()

            @pl.when(jnp.logical_not(by_extra(g, q, col)))
            def _():
                side_copy(g, q, 1 - col).wait_recv()

            attend(g, q, False)

            @pl.when(q == 0)
            def _():
                finish(g)

            return inner

        return lax.fori_loop(0, kv_heads, one, carry)

    lax.fori_loop(2, plane + 2, step, 0)

    mean = jnp.sum(squares[...], axis=1, keepdims=True) / width
    scale = jnp.broadcast_to(lax.rsqrt(mean + norm_eps), (rows, W))
    for head in range(kv_heads * per_group):
        lanes = slice(head * W, (head + 1) * W)
        gain = gain_ref[lanes].reshape(1, W)
        out_ref[0, :, lanes] = (top[head] * scale * gain).astype(jnp.bfloat16)

    def drain_own(g, carry):
        @pl.when(has_up)
        def _():
            up_copy(g, plane).wait_send()

        @pl.when(col == 0)
        def _():
            side_copy(g, plane, col).wait_send()

        @pl.when((col == 1) & has_up & (lax.rem(g, 2) == 1))
        def _():
            extra_copy(g).wait_send()

        return carry

    lax.fori_loop(0, kv_heads, drain_own, 0)

    def drain(q, carry):
        def one(g, inner):
            @pl.when(has_up)
            def _():
                up_copy(g, q).wait_send()

            @pl.when(jnp.logical_not(by_extra(g, q, 1 - col)))
            def _():
                side_copy(g, q, col).wait_send()

            return inner

        return lax.fori_loop(0, kv_heads, one, carry)

    lax.fori_loop(0, plane, drain, 0)


def body(queries, keys, values, residual, norm_gain):
    count = lax.axis_size("seq")
    rows = queries.shape[1]
    width = queries.shape[2]
    kv_heads = keys.shape[2] // HEAD_WIDTH
    heads = width // HEAD_WIDTH
    planes = count // 2
    hbm = pl.BlockSpec(memory_space=pltpu.HBM)
    vmem = pl.BlockSpec(memory_space=pltpu.VMEM)
    return pl.pallas_call(
        functools.partial(kernel, planes, rows, kv_heads, heads // kv_heads),
        out_shape=jax.ShapeDtypeStruct(queries.shape, jnp.bfloat16),
        in_specs=[hbm, hbm, hbm, hbm, vmem],
        out_specs=vmem,
        scratch_shapes=[
            pltpu.VMEM((heads, rows, HEAD_WIDTH), jnp.bfloat16),
            pltpu.VMEM((rows, width), jnp.bfloat16),
            pltpu.VMEM((kv_heads, count, rows, 2 * HEAD_WIDTH), jnp.bfloat16),
            pltpu.VMEM((heads, rows, HEAD_WIDTH), jnp.float32),
            pltpu.VMEM((heads, rows, 2 * HEAD_WIDTH), jnp.float32),
            pltpu.VMEM((rows, HEAD_WIDTH), jnp.float32),
            pltpu.SemaphoreType.DMA((heads + 1,)),
            pltpu.SemaphoreType.DMA((kv_heads, 2)),
            pltpu.SemaphoreType.DMA((kv_heads, planes)),
            pltpu.SemaphoreType.DMA((kv_heads, planes)),
            pltpu.SemaphoreType.DMA((kv_heads, planes)),
            pltpu.SemaphoreType.DMA((kv_heads, planes)),
            pltpu.SemaphoreType.DMA((kv_heads,)),
            pltpu.SemaphoreType.DMA((kv_heads,)),
        ],
        compiler_params=pltpu.CompilerParams(
            collective_id=0, has_side_effects=True, vmem_limit_bytes=67043328
        ),
    )(queries, keys, values, residual, norm_gain)


def solution(mesh):
    rows = P(("groups", "vocab", "batch"), "seq", None)
    return jax.shard_map(
        body,
        mesh=mesh,
        in_specs=(rows, rows, rows, rows, P()),
        out_specs=rows,
        check_vma=False,
    )
```

```python
import functools
import math

import jax
import jax.numpy as jnp
from jax import lax
from jax.experimental import pallas as pl
from jax.experimental.pallas import tpu as pltpu
from jax.sharding import PartitionSpec as P

HEAD_WIDTH = 128
norm_eps = 1e-06
MESH = pl.DeviceIdType.MESH


def kernel(
    planes,
    rows,
    kv_heads,
    per_group,
    q_hbm,
    kv_hbm,
    r_hbm,
    gain_ref,
    out_ref,
    qbuf,
    rbuf,
    kvbuf,
    top,
    acc,
    squares,
    local_sem,
    own_sem,
    up_send,
    up_recv,
    side_send,
    side_recv,
    extra_send,
    extra_recv,
):
    W = HEAD_WIDTH
    width = kv_heads * per_group * W
    me = lax.axis_index("seq")
    plane = me // 2
    col = lax.rem(me, 2)
    above = me + 2
    below = me - 2
    side = me + 1 - 2 * col
    has_up = plane + 1 < planes
    has_down = plane > 0
    factor = math.log2(math.e) / math.sqrt(W)

    own = []
    for g in range(kv_heads):
        copy = pltpu.make_async_copy(kv_hbm.at[g], kvbuf.at[g, me], own_sem.at[g])
        copy.start()
        own.append(copy)
    heads = kv_heads * per_group

    def query_copy(head):
        lanes = pl.ds(pl.multiple_of(head * W, W), W)
        return pltpu.make_async_copy(
            q_hbm.at[0, :, lanes], qbuf.at[head], local_sem.at[head]
        )

    r_in = pltpu.make_async_copy(r_hbm.at[0], rbuf, local_sem.at[heads])

    barrier = pltpu.get_barrier_semaphore()
    pl.semaphore_signal(barrier, inc=1, device_id={"seq": side}, device_id_type=MESH)

    @pl.when(has_up)
    def _():
        pl.semaphore_signal(barrier, inc=1, device_id={"seq": above}, device_id_type=MESH)

    @pl.when(has_down)
    def _():
        pl.semaphore_signal(barrier, inc=1, device_id={"seq": below}, device_id_type=MESH)

    pl.semaphore_wait(barrier, 1 + has_up.astype(jnp.int32) + has_down.astype(jnp.int32))

    def remote(slot, send_sem, recv_sem, target):
        return pltpu.make_async_remote_copy(
            src_ref=slot,
            dst_ref=slot,
            send_sem=send_sem,
            recv_sem=recv_sem,
            device_id={"seq": target},
            device_id_type=MESH,
        )

    def up_copy(g, q):
        return remote(kvbuf.at[g, 2 * q + col], up_send.at[g, q], up_recv.at[g, q], above)

    def side_copy(g, q, column):
        return remote(kvbuf.at[g, 2 * q + column], side_send.at[g, q], side_recv.at[g, q], side)

    def extra_copy(g):
        return remote(kvbuf.at[g, 0], extra_send.at[g], extra_recv.at[g], above)

    def by_extra(g, q, column):
        return (column == 1) & (q == 0) & has_down & (lax.rem(g, 2) == 1)

    for g in range(kv_heads):
        own[g].wait()

        @pl.when(has_up)
        def _(g=g):
            up_copy(g, plane).start()

        @pl.when(col == 0)
        def _(g=g):
            side_copy(g, plane, col).start()

    lax.fori_loop(0, heads, lambda head, carry: query_copy(head).start(), None)
    r_in.start()

    @pl.when(col == 0)
    def _():
        for g in range(kv_heads):
            kvbuf[g, me + 1] = jnp.zeros((rows, 2 * W), jnp.bfloat16)

    squares[...] = jnp.zeros_like(squares)
    lax.fori_loop(0, heads, lambda head, carry: query_copy(head).wait(), None)
    r_in.wait()

    def relay(g, q):
        up_copy(g, q).wait_recv()

        @pl.when(has_up)
        def _():
            up_copy(g, q).start()

        @pl.when(jnp.logical_not(by_extra(g, q, 1 - col)))
        def _():
            side_copy(g, q, col).start()

    def attend(g, q, first):
        keys = kvbuf[g, pl.ds(2 * q, 2), :, :W].reshape(2 * rows, W)
        vals = kvbuf[g, pl.ds(2 * q, 2), :, W:].reshape(2 * rows, W)
        vals = jnp.concatenate([vals, jnp.ones_like(vals)], axis=1)

        def scores(j):
            return lax.dot_general(
                qbuf[g * per_group + j],
                keys,
                (((1,), (1,)), ((), ())),
                preferred_element_type=jnp.float32,
            )

        s_next = scores(0)
        for j in range(per_group):
            head = g * per_group + j
            s = s_next
            if j + 1 < per_group:
                s_next = scores(j + 1)
            if first:
                at_row = lax.broadcasted_iota(jnp.int32, s.shape, 0) + col * rows
                at_key = lax.broadcasted_iota(jnp.int32, s.shape, 1)
                s = jnp.where(at_key <= at_row, s, -jnp.inf)
            wide = jnp.broadcast_to(jnp.max(s, axis=1, keepdims=True), (rows, W))
            if not first:
                old = top[head]
                wide = jnp.maximum(old, wide)
            s = (s - jnp.concatenate([wide] * (2 * rows // W), axis=1)) * factor
            w = jnp.exp2(s).astype(jnp.bfloat16)
            o = jnp.dot(w, vals, preferred_element_type=jnp.float32)
            if not first:
                fade = jnp.exp2((old - wide) * factor)
                o = o + acc[head] * jnp.concatenate([fade, fade], axis=1)
            top[head] = wide
            acc[head] = o

    def finish(g):
        total = squares[...]
        for j in range(per_group):
            head = g * per_group + j
            lanes = pl.ds(pl.multiple_of(head * W, W), W)
            both = acc[head]
            attended = (both[:, :W] / both[:, W:]).astype(jnp.bfloat16).astype(jnp.float32)
            hidden = rbuf[:, lanes].astype(jnp.float32) + attended
            total = total + hidden * hidden
            top[head] = hidden
        squares[...] = total

    def diagonal(g, carry):
        @pl.when(has_down)
        def _():
            relay(g, plane - 1)

        @pl.when(col == 1)
        def _():
            side_copy(g, plane, 1 - col).wait_recv()

        @pl.when((col == 1) & (plane == 0) & has_up & (lax.rem(g, 2) == 1))
        def _():
            extra_copy(g).start()

        attend(g, plane, True)

        @pl.when(plane == 0)
        def _():
            finish(g)

        return carry

    lax.fori_loop(0, kv_heads, diagonal, 0)

    def step(t, carry):
        q = plane - t + 1

        def one(g, inner):
            @pl.when(t <= plane)
            def _():
                relay(g, q - 1)

            @pl.when(by_extra(g, q, col))
            def _():
                extra_copy(g).wait_recv()

            @pl.when(by_extra(g, q, col) & has_up)
            def _():
                extra_copy(g).start()

            @pl.when(jnp.logical_not(by_extra(g, q, col)))
            def _():
                side_copy(g, q, 1 - col).wait_recv()

            attend(g, q, False)

            @pl.when(q == 0)
            def _():
                finish(g)

            return inner

        return lax.fori_loop(0, kv_heads, one, carry)

    lax.fori_loop(2, plane + 2, step, 0)

    mean = jnp.sum(squares[...], axis=1, keepdims=True) / width
    scale = jnp.broadcast_to(lax.rsqrt(mean + norm_eps), (rows, W))
    for head in range(kv_heads * per_group):
        lanes = slice(head * W, (head + 1) * W)
        gain = gain_ref[lanes].reshape(1, W)
        out_ref[0, :, lanes] = (top[head] * scale * gain).astype(jnp.bfloat16)

    def drain_own(g, carry):
        @pl.when(has_up)
        def _():
            up_copy(g, plane).wait_send()

        @pl.when(col == 0)
        def _():
            side_copy(g, plane, col).wait_send()

        @pl.when((col == 1) & has_up & (lax.rem(g, 2) == 1))
        def _():
            extra_copy(g).wait_send()

        return carry

    lax.fori_loop(0, kv_heads, drain_own, 0)

    def drain(q, carry):
        def one(g, inner):
            @pl.when(has_up)
            def _():
                up_copy(g, q).wait_send()

            @pl.when(jnp.logical_not(by_extra(g, q, 1 - col)))
            def _():
                side_copy(g, q, col).wait_send()

            return inner

        return lax.fori_loop(0, kv_heads, one, carry)

    lax.fori_loop(0, plane, drain, 0)


def body(queries, keys, values, residual, norm_gain):
    count = lax.axis_size("seq")
    rows = queries.shape[1]
    width = queries.shape[2]
    kv_heads = keys.shape[2] // HEAD_WIDTH
    heads = width // HEAD_WIDTH
    planes = count // 2
    pairs = jnp.stack(
        [
            jnp.concatenate([x[0, :, g * HEAD_WIDTH : (g + 1) * HEAD_WIDTH] for x in (keys, values)], axis=1)
            for g in range(kv_heads)
        ]
    )
    hbm = pl.BlockSpec(memory_space=pltpu.HBM)
    vmem = pl.BlockSpec(memory_space=pltpu.VMEM)
    return pl.pallas_call(
        functools.partial(kernel, planes, rows, kv_heads, heads // kv_heads),
        out_shape=jax.ShapeDtypeStruct(queries.shape, jnp.bfloat16),
        in_specs=[hbm, hbm, hbm, vmem],
        out_specs=vmem,
        scratch_shapes=[
            pltpu.VMEM((heads, rows, HEAD_WIDTH), jnp.bfloat16),
            pltpu.VMEM((rows, width), jnp.bfloat16),
            pltpu.VMEM((kv_heads, count, rows, 2 * HEAD_WIDTH), jnp.bfloat16),
            pltpu.VMEM((heads, rows, HEAD_WIDTH), jnp.float32),
            pltpu.VMEM((heads, rows, 2 * HEAD_WIDTH), jnp.float32),
            pltpu.VMEM((rows, HEAD_WIDTH), jnp.float32),
            pltpu.SemaphoreType.DMA((heads + 1,)),
            pltpu.SemaphoreType.DMA((kv_heads,)),
            pltpu.SemaphoreType.DMA((kv_heads, planes)),
            pltpu.SemaphoreType.DMA((kv_heads, planes)),
            pltpu.SemaphoreType.DMA((kv_heads, planes)),
            pltpu.SemaphoreType.DMA((kv_heads, planes)),
            pltpu.SemaphoreType.DMA((kv_heads,)),
            pltpu.SemaphoreType.DMA((kv_heads,)),
        ],
        compiler_params=pltpu.CompilerParams(
            collective_id=0, has_side_effects=True, vmem_limit_bytes=54500000
        ),
    )(queries, pairs, residual, norm_gain)


def solution(mesh):
    rows = P(("groups", "vocab", "batch"), "seq", None)
    return jax.shard_map(
        body,
        mesh=mesh,
        in_specs=(rows, rows, rows, rows, P()),
        out_specs=rows,
        check_vma=False,
    )
```
